32 devices in a mesh: gx: 4 (over z), gy: 2 (over y), gz: 4 (over x, core).
Axes of the slice: x: 2, y: 2, z: 4, core: 2. Of those that a mesh axis runs over, the one named last changes fastest.
Arguments:
- start_disp: float32 [3, 32, 16, 512], P(None, 'gx', 'gy', 'gz'), may hold values from -2 to 2
- inertial: float32 [3, 32, 16, 512], P(None, 'gx', 'gy', 'gz'), may hold values from -1 to 1
- material: int32 [32, 16, 512], P('gx', 'gy', 'gz'), may hold values from 0 to 7
- pinned: int32 [32, 16, 512], P('gx', 'gy', 'gz'), may hold values 0 or 1
- stiffness: float32 [8], replicated, may hold values from 3 to 100
Outputs:
- displacement: float32 [3, 32, 16, 512], P(None, 'gx', 'gy', 'gz')
The draws below stay inside these ranges and needn't reach their ends.
All inputs are finite; a program needn't handle non-finite values. No bound on the sum of `pinned` on one device may be relied on, other than what follows from the above.
Results may differ from the reference program's by a relative error of at most 0.0003.
Values sent between devices are 32-bit elements; how exact they have to be, the bound alone decides.
A program may use at most 64 MiB of HBM per device.

```python
import math
import jax
import jax.numpy as jnp
from jax import lax

CX = 8
ITERS = 4
POLAR_STEPS = 6
MATS = 8
NX = 32
NY = 16
NZ = 512


def set_ends(drawn, rng, low, largest):
    spot = [jax.random.randint(jax.random.fold_in(rng, axis), (), 0, length) for axis, length in enumerate(drawn.shape)]
    main_axis = drawn.shape.index(max(drawn.shape))
    next_to = spot[:main_axis] + [(spot[main_axis] + 1) % drawn.shape[main_axis]] + spot[main_axis + 1:]
    return drawn.at[tuple(spot)].set(low).at[tuple(next_to)].set(largest)


def levels(own_key, dims, split, low, largest):
    loudness, own = 1.0, jax.random.fold_in(own_key, 6)
    for position, shards_of in split:
        draws = jnp.exp(jax.random.uniform(jax.random.fold_in(own, position), (shards_of,), jnp.float32, low / len(split), largest / len(split)))
        loudness = loudness * jnp.repeat(draws, dims[position] // shards_of).reshape([-1 if axis == position else 1 for axis in range(len(dims))])
    return loudness


def gaussian(stream_key, extent, spread, most, cuts=(), kind=jnp.bfloat16):
    level = levels(stream_key, extent, cuts, -0.22, 0.18) if cuts else 1.0
    values = jax.random.normal(stream_key, extent, jnp.float32) * spread * level
    return jnp.minimum(jnp.maximum(values, -most), most).astype(kind)


def setup_inputs(seed: int = 0) -> dict:
    key_of = jax.random.split(jax.random.key(seed), 6)
    return {
        "start_disp": gaussian(key_of[0], (3, NX, NY, NZ), 0.5, 2.0, ((1, 4), (2, 2), (3, 4)), jnp.float32),
        "inertial": gaussian(key_of[1], (3, NX, NY, NZ), 0.25, 1.0, ((1, 4), (2, 2), (3, 4)), jnp.float32),
        "material": set_ends(jax.random.randint(key_of[2], (NX, NY, NZ), 0, MATS), jax.random.fold_in(key_of[2], 1), 0, MATS - 1).astype(jnp.int32),
        "pinned": set_ends((jax.random.randint(key_of[3], (NX, NY, NZ), 0, 16) < 1).astype(jnp.int32), jax.random.fold_in(key_of[3], 1), 0, 1),
        "stiffness": jnp.clip(jnp.exp(jax.random.uniform(key_of[4], (MATS,), jnp.float32, math.log(3.0), math.log(100.0))), 3.0, 100.0),
    }


inertia = 1.0
relax = 0.6
radius = 0.9

def forward_diff(field, axis):
    size = field.shape[axis]
    return lax.slice_in_dim(field, 1, size, axis=axis) - lax.slice_in_dim(field, 0, size - 1, axis=axis)

def pair_sum(field, axis):
    size = field.shape[axis]
    return lax.slice_in_dim(field, 1, size, axis=axis) + lax.slice_in_dim(field, 0, size - 1, axis=axis)

def gradient(field, axis):
    result = forward_diff(field, axis)
    for other in range(3):
        if other != axis:
            result = pair_sum(result, other)
    return 0.25 * result

def project(nodes, welem):
    deform = [[gradient(nodes[c], d) + (1.0 if c == d else 0.0) for d in range(3)] for c in range(3)]
    total = sum((deform[c][d] * deform[c][d] for c in range(3) for d in range(3)))
    scale = jnp.maximum(jnp.sqrt(total / 3.0), 1.0)
    rotate = [[deform[c][d] / scale for d in range(3)] for c in range(3)]
    for step in range(POLAR_STEPS):
        middle = [[(1.5 if i == j else 0.0) - 0.5 * sum((rotate[k][i] * rotate[k][j] for k in range(3))) for j in range(3)] for i in range(3)]
        rotate = [[sum((rotate[c][j] * middle[j][d] for j in range(3))) for d in range(3)] for c in range(3)]
    return [welem * (deform[c][d] - rotate[c][d]) for c in range(3) for d in range(3)]

def assemble(stress):
    forces = []
    for c in range(3):
        total = 0.0
        for d in range(3):
            term = stress[3 * c + d]
            for other in range(3):
                if other != d:
                    term = pair_sum(term, other)
            total = total - 0.25 * forward_diff(term, d)
        forces.append(total)
    return jnp.stack(forces)

def diagonal(welem):
    total = welem
    for axis in range(3):
        total = pair_sum(total, axis)
    return inertia + 3.0 / 16.0 * total

def lookup(material, stiffness):
    total = jnp.zeros(material.shape, jnp.float32)
    for index in range(MATS):
        total = total + jnp.where(material == index, stiffness[index], 0.0)
    return total

def reference(start_disp, inertial, material, pinned, stiffness):
    grid_x = lax.broadcasted_iota(jnp.int32, material.shape, 0)
    grid_y = lax.broadcasted_iota(jnp.int32, material.shape, 1)
    grid_z = lax.broadcasted_iota(jnp.int32, material.shape, 2)
    valid = (grid_x < NX - 1) & (grid_y < NY - 1) & (grid_z < NZ - 1)
    weights = jnp.where(valid, lookup(material, stiffness), 0.0)
    welem = jnp.pad(weights, ((1, 0), (1, 0), (1, 0)))
    diag = diagonal(welem)
    pins = pinned[None] > 0
    disp = jnp.where(pins, inertial, start_disp)
    previous = disp
    omega = 1.0
    blocks = NX // CX
    for step in range(ITERS):
        padded = jnp.pad(disp, ((0, 0), (1, 1), (1, 1), (1, 1)))

        def block_forces(index):
            start = (index * CX).astype(jnp.int32)
            nodes = lax.dynamic_slice_in_dim(padded, start, CX + 2, 1)
            wslab = lax.dynamic_slice_in_dim(welem, start, CX + 1, 0)
            return assemble(project([nodes[0], nodes[1], nodes[2]], wslab))
        parts = lax.map(block_forces, jnp.arange(blocks, dtype=jnp.int32))
        forces = jnp.moveaxis(parts, 0, 1).reshape(3, NX, NY, NZ)
        target = disp - relax * (inertia * (disp - inertial) + forces) / diag[None]
        if step == 0:
            fresh = target
        else:
            omega = 2.0 / (2.0 - radius * radius) if step == 1 else 4.0 / (4.0 - radius * radius * omega)
            fresh = omega * (target - previous) + previous
        fresh = jnp.where(pins, inertial, fresh)
        previous = disp
        disp = fresh
    return disp
```

```python
import functools

import jax
import jax.numpy as jnp
from jax import lax
from jax.experimental import pallas as pl
from jax.experimental.pallas import tpu as pltpu
from jax.sharding import PartitionSpec as P

ITERS = 4
POLAR_STEPS = 6
MATS = 8

relax = 0.6
radius = 0.9
HALO = ITERS
SLOT = 2 * HALO
NARR = 8
AXES = ("gx", "gy", "gz")


def node_terms(u, uz, roll_y):
    zs, zd = uz + u, uz - u
    ys, yd = roll_y(zs), roll_y(zd)
    return zs + ys, ys - zs, zd + yd


def stretch(low, high):
    deform = []
    for c in range(3):
        dx = high[c][0] - low[c][0]
        dy = high[c][1] + low[c][1]
        dz = high[c][2] + low[c][2]
        row = [dx, dy, dz]
        row[c] = row[c] + 1.0
        deform.append(row)
    return deform


def stress(deform, w):
    total = None
    for c in range(3):
        for d in range(3):
            sq = deform[c][d] * deform[c][d]
            total = sq if total is None else total + sq
    inv = jnp.minimum(lax.rsqrt(total * (1.0 / 3.0)), 1.0) * (0.5**0.5)
    z = [[deform[c][d] * inv for d in range(3)] for c in range(3)]

    def polar(_, flat):
        z = [flat[3 * c : 3 * c + 3] for c in range(3)]
        s = {}
        for i in range(3):
            for j in range(i, 3):
                s[i, j] = z[0][i] * z[0][j] + z[1][i] * z[1][j] + z[2][i] * z[2][j]
        m = [1.5 - s[i, i] for i in range(3)]
        out = []
        for c in range(3):
            a, b, e = z[c]
            out.append(a * m[0] - b * s[0, 1] - e * s[0, 2])
            out.append(b * m[1] - a * s[0, 1] - e * s[1, 2])
            out.append(e * m[2] - a * s[0, 2] - b * s[1, 2])
        return tuple(out)

    flat = lax.fori_loop(
        0, POLAR_STEPS, polar, tuple(z[c][d] for c in range(3) for d in range(3)), unroll=True
    )
    return [w * (deform[k // 3][k % 3] - flat[k] * (2.0**0.5)) for k in range(9)]


def node_sums(before, here, roll_y):
    a = before[0] - here[0]
    b = before[1] + here[1]
    e = before[2] + here[2]
    g = (a - b) + roll_y(a + b)
    e = e + roll_y(e)
    return g - e, g + e


def advance(u, prev, inert, pin, rate, f, omega):
    target = u - rate * ((u - inert) + f)
    fresh = target if omega is None else omega * (target - prev) + prev
    return jnp.where(pin > 0.0, inert, fresh)


def kernel(
    counts, start, inertial, material, pinned, stiff, out,
    xe, sy, ry, ext, az, rz, prev, rate, terms, press, strip, sprev, srate, hz,
    send_sem, recv_sem,
):
    size_x, size_y, size_z = material.shape
    here = [lax.axis_index(a) for a in AXES]
    has = [[here[i] > 0, here[i] < counts[i] - 1] for i in range(3)]

    sub = lax.broadcasted_iota(jnp.int32, (size_y, size_z), 0)
    lane = lax.broadcasted_iota(jnp.int32, (size_y, size_z), 1)
    inside = ((sub < size_y - 1) | has[1][1]) & ((lane < size_z - 1) | has[2][1])
    quarter = [stiff[i] * 0.25 for i in range(MATS)]

    barrier = pltpu.get_barrier_semaphore()

    def peer(i, side):
        return {AXES[i]: here[i] + (1 if side else -1)}

    for i in range(3):
        for side in range(2):
            @pl.when(has[i][side])
            def _(i=i, side=side):
                pl.semaphore_signal(
                    barrier, inc=1, device_id=peer(i, side), device_id_type=pl.DeviceIdType.MESH
                )

    def pack_y(x, _):
        for p in range(NARR // 2):
            first, second = xe[2 * p, x], xe[2 * p + 1, x]
            low = jnp.where(sub < HALO, first, pltpu.roll(second, HALO, 0))
            high = jnp.where(sub < HALO, pltpu.roll(first, HALO, 0), second)
            sy[0, p, x] = low
            sy[1, p, x] = high
        return 0

    def own_plane(x, _):
        mat = material[x]
        w = jnp.zeros((size_y, size_z), jnp.float32)
        for index in range(MATS):
            w = jnp.where(mat == index, quarter[index], w)
        keep = inside & ((x < size_x - 1) | has[0][1])
        xe[6, x + HALO] = jnp.where(keep, w, 0.0)
        pins = pinned[x] > 0
        xe[7, x + HALO] = jnp.where(pins, 1.0, 0.0)
        for c in range(3):
            inert = inertial[c, x]
            xe[3 + c, x + HALO] = inert
            xe[c, x + HALO] = jnp.where(pins, inert, start[c, x])
        pack_y(x + HALO, 0)
        return 0

    lax.fori_loop(0, size_x, own_plane, 0)

    def zero(ref, lo, n):
        def body(x, _):
            for a in range(ref.shape[0]):
                ref[a, x] = jnp.zeros(ref.shape[2:], jnp.float32)
            return 0
        lax.fori_loop(lo, lo + n, body, 0)

    top = HALO + size_x
    for side, lo in ((0, 0), (1, top)):
        @pl.when(jnp.logical_not(has[0][side]))
        def _(lo=lo):
            zero(xe, lo, HALO)
    for side in range(2):
        @pl.when(jnp.logical_not(has[1][side]))
        def _(side=side):
            zero(ry.at[side], 0, top + HALO)

    n = 0
    for i in range(3):
        for side in range(2):
            n = n + has[i][side].astype(jnp.int32)
    pl.semaphore_wait(barrier, n)

    def remote(src, dst, k, i, side):
        return pltpu.make_async_remote_copy(
            src_ref=src, dst_ref=dst, send_sem=send_sem.at[k], recv_sem=recv_sem.at[k],
            device_id=peer(i, side), device_id_type=pl.DeviceIdType.MESH,
        )

    def x_copy(side):
        src = xe.at[:, pl.ds(HALO if side == 0 else size_x, HALO)]
        dst = xe.at[:, pl.ds(top if side == 0 else 0, HALO)]
        return remote(src, dst, side, 0, side)

    def y_copy(side, part):
        lo, count = ((0, HALO), (HALO, size_x), (top, HALO))[part]
        return remote(
            sy.at[side, :, pl.ds(lo, count)], ry.at[1 - side, :, pl.ds(lo, count)],
            2 + 3 * side + part, 1, side,
        )

    def z_copy(side):
        return remote(az.at[side], rz.at[1 - side], 8 + side, 2, side)

    def each(i, action):
        for side in range(2):
            @pl.when(has[i][side])
            def _(side=side):
                action(side)

    each(0, lambda side: x_copy(side).start())
    each(1, lambda side: y_copy(side, 1).start())
    each(0, lambda side: x_copy(1 - side).wait_recv())
    lax.fori_loop(0, HALO, pack_y, 0)
    lax.fori_loop(top, top + HALO, pack_y, 0)
    each(1, lambda side: (y_copy(side, 0).start(), y_copy(side, 2).start()))

    wide = lax.broadcasted_iota(jnp.int32, (2 * HALO + size_y, size_z), 1)

    def fill(x, _):
        for p in range(NARR // 2):
            lo, hi = ry[0, p, x], ry[1, p, x]
            for q in range(2):
                a = 2 * p + q
                own = pltpu.roll(xe[a, x], HALO, 0)
                lo_part = lo if q == 0 else pltpu.roll(lo, HALO, 0)
                hi_part = hi if q == 1 else pltpu.roll(hi, HALO, 0)
                ext[a, x, 0:size_y] = jnp.where(sub < HALO, lo_part, own)
                ext[a, x, size_y : 2 * size_y] = jnp.where(sub < HALO, own, hi_part)
        return 0

    each(1, lambda side: y_copy(1 - side, 1).wait_recv())
    lax.fori_loop(HALO, top, fill, 0)
    each(1, lambda side: (y_copy(1 - side, 0).wait_recv(), y_copy(1 - side, 2).wait_recv()))
    lax.fori_loop(0, HALO, fill, 0)
    lax.fori_loop(top, top + HALO, fill, 0)

    planes = top + HALO

    def pack_z(a, _):
        low = jnp.zeros(wide.shape, jnp.float32)
        high = low
        for x in range(planes):
            spot = (wide >= x * SLOT) & (wide < (x + 1) * SLOT)
            plane = ext[a, x]
            low = jnp.where(spot, pltpu.roll(plane, (x * SLOT + HALO) % size_z, 1), low)
            high = jnp.where(spot, pltpu.roll(plane, (x * SLOT + HALO) % size_z, 1), high)
        az[0, a] = low
        az[1, a] = high
        return 0

    lax.fori_loop(0, NARR, pack_z, 0)
    each(2, lambda side: z_copy(side).start())
    for side in range(2):
        @pl.when(jnp.logical_not(has[2][side]))
        def _(side=side):
            for a in range(NARR):
                rz[side, a] = jnp.zeros(wide.shape, jnp.float32)
    each(2, lambda side: z_copy(1 - side).wait_recv())

    early = lax.rem(wide, SLOT) < HALO
    for a in range(NARR):
        strip[0, a] = jnp.where(early, rz[0, a], az[0, a])
        strip[1, a] = jnp.where(early, az[1, a], rz[1, a])

    rows = 2 * HALO + size_y
    up = lambda v: pltpu.roll(v, rows - 1, 0)
    down = lambda v: pltpu.roll(v, 1, 0)
    zup = lambda v: pltpu.roll(v, size_z - 1, 1)
    zdown = lambda v: pltpu.roll(v, 1, 1)
    xup = lambda v: pltpu.roll(v, size_z - SLOT, 1)
    xdown = lambda v: pltpu.roll(v, SLOT, 1)

    def speed(total):
        return relax / (1.0 + 0.75 * total)

    for s in range(2):
        w = strip[s, 6]
        w = w + xdown(w)
        w = w + down(w)
        if s == 0:
            hz[0] = w
        srate[s] = speed(w + zdown(w))
        for c in range(3):
            sprev[s, c] = strip[s, c]

    first_lane = wide == 0
    last_lane = wide == size_z - 1

    def from_low(v, x):
        return pltpu.roll(v, size_z - HALO + 1 - SLOT * x, 1)

    def from_high(v, x):
        return pltpu.roll(v, size_z - 1 - HALO - SLOT * x, 1)

    def store_terms(x, c, u):
        uz = jnp.where(last_lane, from_high(strip[1, c], x), zup(u))
        for k, term in enumerate(node_terms(u * 0.25, uz * 0.25, up)):
            terms[x, 3 * c + k] = term

    def setup(x, _):
        for c in range(3):
            u = ext[c, x]
            prev[c, x] = u
            store_terms(x, c, u)
        return 0

    def setup_rate(x, _):
        w = ext[6, x - 1] + ext[6, x]
        w = w + down(w)
        rate[x] = speed(w + jnp.where(first_lane, from_low(hz[0], x), zdown(w)))
        return 0

    lax.fori_loop(0, planes, setup, 0)
    lax.fori_loop(1, planes - 1, setup_rate, 0)

    omega = None
    for step in range(ITERS):
        if step == 1:
            omega = 2.0 / (2.0 - radius * radius)
        elif step > 1:
            omega = 4.0 / (4.0 - radius * radius * omega)
        last = step == ITERS - 1

        def strips(s, _):
            low, high = [], []
            for c in range(3):
                u = strip[s, c] * 0.25
                t = node_terms(u, zup(u), up)
                low.append(t)
                high.append([xup(v) for v in t])
            p = stress(stretch(low, high), strip[s, 6])
            for c in range(3):
                mine = p[3 * c : 3 * c + 3]
                minus, plus = node_sums([xdown(v) for v in mine], mine, down)
                hz[3 * s + c] = plus
                u = strip[s, c]
                fresh = advance(
                    u, sprev[s, c], strip[s, 3 + c], strip[s, 7], srate[s],
                    minus + zdown(plus), omega,
                )
                sprev[s, c] = u
                strip[s, c] = fresh
            return 0

        def voxels(x, _):
            low = [[terms[x, 3 * c + k] for k in range(3)] for c in range(3)]
            high = [[terms[x + 1, 3 * c + k] for k in range(3)] for c in range(3)]
            p = stress(stretch(low, high), ext[6, x])
            for k in range(9):
                press[x, k] = p[k]
            return 0

        def nodes(x, _):
            for c in range(3):
                minus, plus = node_sums(
                    [press[x - 1, 3 * c + k] for k in range(3)],
                    [press[x, 3 * c + k] for k in range(3)],
                    down,
                )
                f = minus + jnp.where(first_lane, from_low(hz[c], x), zdown(plus))
                u = ext[c, x]
                fresh = advance(u, prev[c, x], ext[3 + c, x], ext[7, x], rate[x], f, omega)
                if last:
                    out[c, x - HALO] = fresh[HALO : HALO + size_y]
                else:
                    prev[c, x] = u
                    ext[c, x] = fresh
                    store_terms(x, c, fresh)
            return 0

        lax.fori_loop(0, 2, strips, 0)
        lax.fori_loop(step, planes - 1 - step, voxels, 0)
        lax.fori_loop(step + 1, planes - 1 - step, nodes, 0)

    each(0, lambda side: x_copy(side).wait_send())
    each(1, lambda side: [y_copy(side, part).wait_send() for part in range(3)])
    each(2, lambda side: z_copy(side).wait_send())


def per_device(counts, start_disp, inertial, material, pinned, stiffness):
    size_x, size_y, size_z = material.shape
    planes, rows = size_x + 2 * HALO, size_y + 2 * HALO
    assert planes * SLOT == size_z and size_y == 2 * HALO
    vmem = pl.BlockSpec(memory_space=pltpu.VMEM)
    f32 = lambda *shape: pltpu.VMEM(shape, jnp.float32)
    return pl.pallas_call(
        functools.partial(kernel, counts),
        out_shape=jax.ShapeDtypeStruct(start_disp.shape, jnp.float32),
        in_specs=[vmem, vmem, vmem, vmem, pl.BlockSpec(memory_space=pltpu.SMEM)],
        out_specs=vmem,
        scratch_shapes=[
            f32(NARR, planes, size_y, size_z),
            f32(2, NARR // 2, planes, size_y, size_z),
            f32(2, NARR // 2, planes, size_y, size_z),
            f32(NARR, planes, rows, size_z),
            f32(2, NARR, rows, size_z),
            f32(2, NARR, rows, size_z),
            f32(3, planes, rows, size_z),
            f32(planes, rows, size_z),
            f32(planes, 9, rows, size_z),
            f32(planes, 9, rows, size_z),
            f32(2, NARR, rows, size_z),
            f32(2, 3, rows, size_z),
            f32(2, rows, size_z),
            f32(6, rows, size_z),
            pltpu.SemaphoreType.DMA((10,)),
            pltpu.SemaphoreType.DMA((10,)),
        ],
        compiler_params=pltpu.CompilerParams(collective_id=0, has_side_effects=True),
    )(start_disp, inertial, material, pinned, stiffness)


def solution(mesh):
    placed = (
        P(None, "gx", "gy", "gz"),
        P(None, "gx", "gy", "gz"),
        P("gx", "gy", "gz"),
        P("gx", "gy", "gz"),
        P(),
    )
    counts = tuple(mesh.shape[a] for a in AXES)
    return jax.shard_map(
        functools.partial(per_device, counts), mesh=mesh, in_specs=placed,
        out_specs=P(None, "gx", "gy", "gz"), check_vma=False,
    )
```

```python
import functools

import jax
import jax.numpy as jnp
from jax import lax
from jax.experimental import pallas as pl
from jax.experimental.pallas import tpu as pltpu
from jax.sharding import PartitionSpec as P

ITERS = 4
POLAR_STEPS = 6
MATS = 8

relax = 0.6
radius = 0.9
HALO = ITERS
SLOT = 2 * HALO
NARR = 8
GROUPS = 2
PAIRS = NARR // 2 // GROUPS
AXES = ("gx", "gy", "gz")


def loop(lo, hi, body, unroll=2):
    assert (hi - lo) % unroll == 0

    def group(k, _):
        body([lo + k * unroll + i for i in range(unroll)])
        return 0

    lax.fori_loop(0, (hi - lo) // unroll, group, 0)


def node_terms(u, uz, roll_y):
    zs, zd = uz + u, uz - u
    ys, yd = roll_y(zs), roll_y(zd)
    return zs + ys, ys - zs, zd + yd


def stretch(low, high):
    deform = []
    for c in range(3):
        dx = high[c][0] - low[c][0]
        dy = high[c][1] + low[c][1]
        dz = high[c][2] + low[c][2]
        row = [dx, dy, dz]
        row[c] = row[c] + 1.0
        deform.append(row)
    return deform


def stress(deform, w):
    total = None
    for c in range(3):
        for d in range(3):
            sq = deform[c][d] * deform[c][d]
            total = sq if total is None else total + sq
    inv = jnp.minimum(lax.rsqrt(total * (1.0 / 3.0)), 1.0) * (0.5**0.5)
    z = [[deform[c][d] * inv for d in range(3)] for c in range(3)]

    def polar(_, flat):
        z = [flat[3 * c : 3 * c + 3] for c in range(3)]
        s = {}
        for i in range(3):
            for j in range(i, 3):
                s[i, j] = z[0][i] * z[0][j] + z[1][i] * z[1][j] + z[2][i] * z[2][j]
        m = [1.5 - s[i, i] for i in range(3)]
        out = []
        for c in range(3):
            a, b, e = z[c]
            out.append(a * m[0] - b * s[0, 1] - e * s[0, 2])
            out.append(b * m[1] - a * s[0, 1] - e * s[1, 2])
            out.append(e * m[2] - a * s[0, 2] - b * s[1, 2])
        return tuple(out)

    flat = lax.fori_loop(
        0, POLAR_STEPS, polar, tuple(z[c][d] for c in range(3) for d in range(3)), unroll=True
    )
    return [w * (deform[k // 3][k % 3] - flat[k] * (2.0**0.5)) for k in range(9)]


def node_sums(before, here, roll_y):
    a = before[0] - here[0]
    b = before[1] + here[1]
    e = before[2] + here[2]
    g = (a - b) + roll_y(a + b)
    e = e + roll_y(e)
    return g - e, g + e


def advance(u, prev, inert, pin, rate, f, omega):
    target = u - rate * ((u - inert) + f)
    fresh = target if omega is None else omega * (target - prev) + prev
    return jnp.where(pin > 0.0, inert, fresh)


def kernel(
    counts, start, inertial, material, pinned, stiff, out,
    xe, sy, ry, ext, az, rz, prev, rate, terms, press, strip, sprev, srate, hz,
    send_sem, recv_sem,
):
    size_x, size_y, size_z = material.shape
    here = [lax.axis_index(a) for a in AXES]
    has = [[here[i] > 0, here[i] < counts[i] - 1] for i in range(3)]

    sub = lax.broadcasted_iota(jnp.int32, (size_y, size_z), 0)
    lane = lax.broadcasted_iota(jnp.int32, (size_y, size_z), 1)
    inside = ((sub < size_y - 1) | has[1][1]) & ((lane < size_z - 1) | has[2][1])
    quarter = [stiff[i] * 0.25 for i in range(MATS)]

    barrier = pltpu.get_barrier_semaphore()

    def peer(i, side):
        return {AXES[i]: here[i] + (1 if side else -1)}

    for i in range(3):
        for side in range(2):
            @pl.when(has[i][side])
            def _(i=i, side=side):
                pl.semaphore_signal(
                    barrier, inc=1, device_id=peer(i, side), device_id_type=pl.DeviceIdType.MESH
                )

    def faces(first, second):
        low = jnp.where(sub < HALO, first, pltpu.roll(second, HALO, 0))
        high = jnp.where(sub < HALO, pltpu.roll(first, HALO, 0), second)
        return low, high

    def pack_y(group, xs):
        done = [
            (p, x, faces(xe[2 * p, x], xe[2 * p + 1, x]))
            for x in xs for p in range(group * PAIRS, (group + 1) * PAIRS)
        ]
        for p, x, (low, high) in done:
            sy[0, p, x] = low
            sy[1, p, x] = high

    def own_planes(xs):
        done = []
        for x in xs:
            mat = material[x]
            w = jnp.zeros((size_y, size_z), jnp.float32)
            for index in range(MATS):
                w = jnp.where(mat == index, quarter[index], w)
            keep = inside & ((x < size_x - 1) | has[0][1])
            pins = pinned[x] > 0
            inert = [inertial[c, x] for c in range(3)]
            arrays = [jnp.where(pins, inert[c], start[c, x]) for c in range(3)] + inert
            arrays += [jnp.where(keep, w, 0.0), jnp.where(pins, 1.0, 0.0)]
            done.append((x + HALO, arrays))
        for x, arrays in done:
            for a in range(NARR):
                xe[a, x] = arrays[a]
            for p in range(NARR // 2):
                low, high = faces(arrays[2 * p], arrays[2 * p + 1])
                sy[0, p, x] = low
                sy[1, p, x] = high

    loop(0, size_x, own_planes)

    def zero(ref, lo, n):
        def body(x, _):
            for a in range(ref.shape[0]):
                ref[a, x] = jnp.zeros(ref.shape[2:], jnp.float32)
            return 0
        lax.fori_loop(lo, lo + n, body, 0)

    top = HALO + size_x
    for side, lo in ((0, 0), (1, top)):
        @pl.when(jnp.logical_not(has[0][side]))
        def _(lo=lo):
            zero(xe, lo, HALO)
    for side in range(2):
        @pl.when(jnp.logical_not(has[1][side]))
        def _(side=side):
            zero(ry.at[side], 0, top + HALO)

    n = 0
    for i in range(3):
        for side in range(2):
            n = n + has[i][side].astype(jnp.int32)
    pl.semaphore_wait(barrier, n)

    def remote(src, dst, k, i, side):
        return pltpu.make_async_remote_copy(
            src_ref=src, dst_ref=dst, send_sem=send_sem.at[k], recv_sem=recv_sem.at[k],
            device_id=peer(i, side), device_id_type=pl.DeviceIdType.MESH,
        )

    def x_copy(side, group):
        span = pl.ds(2 * PAIRS * group, 2 * PAIRS)
        src = xe.at[span, pl.ds(HALO if side == 0 else size_x, HALO)]
        dst = xe.at[span, pl.ds(top if side == 0 else 0, HALO)]
        return remote(src, dst, 2 * group + side, 0, side)

    def y_copy(side, part, group):
        lo, count = ((0, HALO), (HALO, size_x), (top, HALO))[part]
        span = pl.ds(PAIRS * group, PAIRS)
        return remote(
            sy.at[side, span, pl.ds(lo, count)], ry.at[1 - side, span, pl.ds(lo, count)],
            2 * GROUPS + (2 * part + side) * GROUPS + group, 1, side,
        )

    def z_copy(side):
        return remote(az, rz.at[1 - side], 8 * GROUPS + side, 2, side)

    def each(i, action):
        for side in range(2):
            @pl.when(has[i][side])
            def _(side=side):
                action(side)

    for group in range(GROUPS):
        each(0, lambda side: x_copy(side, group).start())
        each(1, lambda side: y_copy(side, 1, group).start())
    for group in range(GROUPS):
        each(0, lambda side: x_copy(1 - side, group).wait_recv())
        loop(0, HALO, functools.partial(pack_y, group))
        loop(top, top + HALO, functools.partial(pack_y, group))
        for part in (0, 2):
            each(1, lambda side: y_copy(side, part, group).start())

    wide = lax.broadcasted_iota(jnp.int32, (2 * HALO + size_y, size_z), 1)

    def fill(xs):
        done = []
        for x in xs:
            for p in range(NARR // 2):
                lo, hi = ry[0, p, x], ry[1, p, x]
                for q in range(2):
                    a = 2 * p + q
                    own = pltpu.roll(xe[a, x], HALO, 0)
                    lo_part = lo if q == 0 else pltpu.roll(lo, HALO, 0)
                    hi_part = hi if q == 1 else pltpu.roll(hi, HALO, 0)
                    done.append((
                        a, x, jnp.where(sub < HALO, lo_part, own),
                        jnp.where(sub < HALO, own, hi_part),
                    ))
        for a, x, low, high in done:
            ext[a, x, 0:size_y] = low
            ext[a, x, size_y : 2 * size_y] = high

    def arrived(part):
        for group in range(GROUPS):
            each(1, lambda side: y_copy(1 - side, part, group).wait_recv())

    arrived(1)
    loop(HALO, top, fill)
    arrived(0)
    arrived(2)
    loop(0, HALO, fill)
    loop(top, top + HALO, fill)

    planes = top + HALO

    def pack_z(a, _):
        packed = jnp.zeros(wide.shape, jnp.float32)
        for x in range(planes):
            spot = (wide >= x * SLOT) & (wide < (x + 1) * SLOT)
            packed = jnp.where(spot, pltpu.roll(ext[a, x], (x * SLOT + HALO) % size_z, 1), packed)
        az[a] = packed
        return 0

    lax.fori_loop(0, NARR, pack_z, 0)
    each(2, lambda side: z_copy(side).start())
    for side in range(2):
        @pl.when(jnp.logical_not(has[2][side]))
        def _(side=side):
            for a in range(NARR):
                rz[side, a] = jnp.zeros(wide.shape, jnp.float32)
    each(2, lambda side: z_copy(1 - side).wait_recv())

    early = lax.rem(wide, SLOT) < HALO
    for a in range(NARR):
        strip[0, a] = jnp.where(early, rz[0, a], az[a])
        strip[1, a] = jnp.where(early, az[a], rz[1, a])

    rows = 2 * HALO + size_y
    up = lambda v: pltpu.roll(v, rows - 1, 0)
    down = lambda v: pltpu.roll(v, 1, 0)
    zup = lambda v: pltpu.roll(v, size_z - 1, 1)
    zdown = lambda v: pltpu.roll(v, 1, 1)
    xup = lambda v: pltpu.roll(v, size_z - SLOT, 1)
    xdown = lambda v: pltpu.roll(v, SLOT, 1)

    def speed(total):
        return relax / (1.0 + 0.75 * total)

    for s in range(2):
        w = strip[s, 6]
        w = w + xdown(w)
        w = w + down(w)
        if s == 0:
            hz[0] = w
        srate[s] = speed(w + zdown(w))
        for c in range(3):
            sprev[s, c] = strip[s, c]

    first_lane = wide == 0
    last_lane = wide == size_z - 1

    def from_low(v, x):
        return pltpu.roll(v, size_z - HALO + 1 - SLOT * x, 1)

    def from_high(v, x):
        return pltpu.roll(v, size_z - 1 - HALO - SLOT * x, 1)

    def make_terms(x, c, u):
        uz = jnp.where(last_lane, from_high(strip[1, c], x), zup(u))
        return node_terms(u * 0.25, uz * 0.25, up)

    def put_terms(done):
        for x, c, three in done:
            for k in range(3):
                terms[x, 3 * c + k] = three[k]

    def setup(xs):
        us = [(x, c, ext[c, x]) for x in xs for c in range(3)]
        done = [(x, c, make_terms(x, c, u)) for x, c, u in us]
        for x, c, u in us:
            prev[c, x] = u
        put_terms(done)

    def setup_rate(xs):
        done = []
        for x in xs:
            w = ext[6, x - 1] + ext[6, x]
            w = w + down(w)
            done.append(speed(w + jnp.where(first_lane, from_low(hz[0], x), zdown(w))))
        for x, r in zip(xs, done):
            rate[x] = r

    loop(0, planes, setup)
    loop(1, planes - 1, setup_rate)

    omega = None
    for step in range(ITERS):
        if step == 1:
            omega = 2.0 / (2.0 - radius * radius)
        elif step > 1:
            omega = 4.0 / (4.0 - radius * radius * omega)
        last = step == ITERS - 1

        def strips(s, _):
            low, high = [], []
            for c in range(3):
                u = strip[s, c] * 0.25
                t = node_terms(u, zup(u), up)
                low.append(t)
                high.append([xup(v) for v in t])
            p = stress(stretch(low, high), strip[s, 6])
            for c in range(3):
                mine = p[3 * c : 3 * c + 3]
                minus, plus = node_sums([xdown(v) for v in mine], mine, down)
                hz[3 * s + c] = plus
                u = strip[s, c]
                fresh = advance(
                    u, sprev[s, c], strip[s, 3 + c], strip[s, 7], srate[s],
                    minus + zdown(plus), omega,
                )
                sprev[s, c] = u
                strip[s, c] = fresh
            return 0

        def voxels(x, _):
            low = [[terms[x, 3 * c + k] for k in range(3)] for c in range(3)]
            high = [[terms[x + 1, 3 * c + k] for k in range(3)] for c in range(3)]
            p = stress(stretch(low, high), ext[6, x])
            for k in range(9):
                press[x, k] = p[k]
            return 0

        def nodes(xs):
            done = []
            for x in xs:
                for c in range(3):
                    minus, plus = node_sums(
                        [press[x - 1, 3 * c + k] for k in range(3)],
                        [press[x, 3 * c + k] for k in range(3)],
                        down,
                    )
                    f = minus + jnp.where(first_lane, from_low(hz[c], x), zdown(plus))
                    u = ext[c, x]
                    fresh = advance(u, prev[c, x], ext[3 + c, x], ext[7, x], rate[x], f, omega)
                    done.append((x, c, u, fresh))
            if last:
                for x, c, _, fresh in done:
                    out[c, x - HALO] = fresh[HALO : HALO + size_y]
                return
            later = [(x, c, make_terms(x, c, fresh)) for x, c, _, fresh in done]
            for x, c, u, fresh in done:
                prev[c, x] = u
                ext[c, x] = fresh
            put_terms(later)

        lax.fori_loop(0, 2, strips, 0)
        lax.fori_loop(step, planes - 1 - step, voxels, 0)
        loop(step + 1, planes - 1 - step, nodes)

    for group in range(GROUPS):
        each(0, lambda side: x_copy(side, group).wait_send())
        for part in range(3):
            each(1, lambda side: y_copy(side, part, group).wait_send())
    each(2, lambda side: z_copy(side).wait_send())


def per_device(counts, start_disp, inertial, material, pinned, stiffness):
    size_x, size_y, size_z = material.shape
    planes, rows = size_x + 2 * HALO, size_y + 2 * HALO
    assert planes * SLOT == size_z and size_y == 2 * HALO
    vmem = pl.BlockSpec(memory_space=pltpu.VMEM)
    f32 = lambda *shape: pltpu.VMEM(shape, jnp.float32)
    return pl.pallas_call(
        functools.partial(kernel, counts),
        out_shape=jax.ShapeDtypeStruct(start_disp.shape, jnp.float32),
        in_specs=[vmem, vmem, vmem, vmem, pl.BlockSpec(memory_space=pltpu.SMEM)],
        out_specs=vmem,
        scratch_shapes=[
            f32(NARR, planes, size_y, size_z),
            f32(2, NARR // 2, planes, size_y, size_z),
            f32(2, NARR // 2, planes, size_y, size_z),
            f32(NARR, planes, rows, size_z),
            f32(NARR, rows, size_z),
            f32(2, NARR, rows, size_z),
            f32(3, planes, rows, size_z),
            f32(planes, rows, size_z),
            f32(planes, 9, rows, size_z),
            f32(planes, 9, rows, size_z),
            f32(2, NARR, rows, size_z),
            f32(2, 3, rows, size_z),
            f32(2, rows, size_z),
            f32(6, rows, size_z),
            pltpu.SemaphoreType.DMA((8 * GROUPS + 2,)),
            pltpu.SemaphoreType.DMA((8 * GROUPS + 2,)),
        ],
        compiler_params=pltpu.CompilerParams(collective_id=0, has_side_effects=True),
    )(start_disp, inertial, material, pinned, stiffness)


def solution(mesh):
    placed = (
        P(None, "gx", "gy", "gz"),
        P(None, "gx", "gy", "gz"),
        P("gx", "gy", "gz"),
        P("gx", "gy", "gz"),
        P(),
    )
    counts = tuple(mesh.shape[a] for a in AXES)
    return jax.shard_map(
        functools.partial(per_device, counts), mesh=mesh, in_specs=placed,
        out_specs=P(None, "gx", "gy", "gz"), check_vma=False,
    )
```

```python
import functools

import jax
import jax.numpy as jnp
from jax import lax
from jax.experimental import pallas as pl
from jax.experimental.pallas import tpu as pltpu
from jax.sharding import PartitionSpec as P

ITERS = 4
POLAR_STEPS = 6
MATS = 8

relax = 0.6
radius = 0.9
HALO = ITERS
SLOT = 2 * HALO
NARR = 8
GROUPS = 2
PAIRS = NARR // 2 // GROUPS
AXES = ("gx", "gy", "gz")


def loop(lo, hi, body, unroll=2):
    assert (hi - lo) % unroll == 0

    def group(k, _):
        body([lo + k * unroll + i for i in range(unroll)])
        return 0

    lax.fori_loop(0, (hi - lo) // unroll, group, 0)


def node_terms(u, uz, roll_y):
    zs, zd = uz + u, uz - u
    ys, yd = roll_y(zs), roll_y(zd)
    return zs + ys, ys - zs, zd + yd


def stretch(low, high):
    deform = []
    for c in range(3):
        dx = high[c][0] - low[c][0]
        dy = high[c][1] + low[c][1]
        dz = high[c][2] + low[c][2]
        row = [dx, dy, dz]
        row[c] = row[c] + 1.0
        deform.append(row)
    return deform


def stress(deform, w):
    total = None
    for c in range(3):
        for d in range(3):
            sq = deform[c][d] * deform[c][d]
            total = sq if total is None else total + sq
    inv = jnp.minimum(lax.rsqrt(total * (1.0 / 3.0)), 1.0) * (0.5**0.5)
    z = [[deform[c][d] * inv for d in range(3)] for c in range(3)]

    def polar(_, flat):
        z = [flat[3 * c : 3 * c + 3] for c in range(3)]
        s = {}
        for i in range(3):
            for j in range(i, 3):
                s[i, j] = z[0][i] * z[0][j] + z[1][i] * z[1][j] + z[2][i] * z[2][j]
        m = [1.5 - s[i, i] for i in range(3)]
        out = []
        for c in range(3):
            a, b, e = z[c]
            out.append(a * m[0] - b * s[0, 1] - e * s[0, 2])
            out.append(b * m[1] - a * s[0, 1] - e * s[1, 2])
            out.append(e * m[2] - a * s[0, 2] - b * s[1, 2])
        return tuple(out)

    flat = lax.fori_loop(
        0, POLAR_STEPS, polar, tuple(z[c][d] for c in range(3) for d in range(3)), unroll=True
    )
    return [w * (deform[k // 3][k % 3] - flat[k] * (2.0**0.5)) for k in range(9)]


def node_sums(before, here, roll_y):
    a = before[0] - here[0]
    b = before[1] + here[1]
    e = before[2] + here[2]
    g = (a - b) + roll_y(a + b)
    e = e + roll_y(e)
    return g - e, g + e


def advance(u, prev, inert, pin, rate, f, omega):
    target = u - rate * ((u - inert) + f)
    fresh = target if omega is None else omega * (target - prev) + prev
    return jnp.where(pin > 0.0, inert, fresh)


def kernel(
    counts, start, inertial, material, pinned, stiff, out,
    xe, sy, ry, ext, az, rz, prev, rate, terms, press, strip, sprev, srate, hz,
    send_sem, recv_sem,
):
    size_x, size_y, size_z = material.shape
    here = [lax.axis_index(a) for a in AXES]
    has = [[here[i] > 0, here[i] < counts[i] - 1] for i in range(3)]

    sub = lax.broadcasted_iota(jnp.int32, (size_y, size_z), 0)
    lane = lax.broadcasted_iota(jnp.int32, (size_y, size_z), 1)
    inside = ((sub < size_y - 1) | has[1][1]) & ((lane < size_z - 1) | has[2][1])
    quarter = [stiff[i] * 0.25 for i in range(MATS)]

    barrier = pltpu.get_barrier_semaphore()

    def peer(i, side):
        return {AXES[i]: here[i] + (1 if side else -1)}

    for i in range(3):
        for side in range(2):
            @pl.when(has[i][side])
            def _(i=i, side=side):
                pl.semaphore_signal(
                    barrier, inc=1, device_id=peer(i, side), device_id_type=pl.DeviceIdType.MESH
                )

    def faces(first, second):
        low = jnp.where(sub < HALO, first, pltpu.roll(second, HALO, 0))
        high = jnp.where(sub < HALO, pltpu.roll(first, HALO, 0), second)
        return low, high

    def pack_y(group, xs):
        done = [
            (p, x, faces(xe[2 * p, x], xe[2 * p + 1, x]))
            for x in xs for p in range(group * PAIRS, (group + 1) * PAIRS)
        ]
        for p, x, (low, high) in done:
            sy[0, p, x] = low
            sy[1, p, x] = high

    def own_planes(xs):
        done = []
        for x in xs:
            mat = material[x]
            w = jnp.zeros((size_y, size_z), jnp.float32)
            for index in range(MATS):
                w = jnp.where(mat == index, quarter[index], w)
            keep = inside & ((x < size_x - 1) | has[0][1])
            pins = pinned[x] > 0
            inert = [inertial[c, x] for c in range(3)]
            arrays = [jnp.where(pins, inert[c], start[c, x]) for c in range(3)] + inert
            arrays += [jnp.where(keep, w, 0.0), jnp.where(pins, 1.0, 0.0)]
            done.append((x + HALO, arrays))
        for x, arrays in done:
            for a in range(NARR):
                xe[a, x] = arrays[a]
            for p in range(NARR // 2):
                low, high = faces(arrays[2 * p], arrays[2 * p + 1])
                sy[0, p, x] = low
                sy[1, p, x] = high

    loop(0, size_x, own_planes)

    def zero(ref, lo, n):
        def body(x, _):
            for a in range(ref.shape[0]):
                ref[a, x] = jnp.zeros(ref.shape[2:], jnp.float32)
            return 0
        lax.fori_loop(lo, lo + n, body, 0)

    top = HALO + size_x
    for side, lo in ((0, 0), (1, top)):
        @pl.when(jnp.logical_not(has[0][side]))
        def _(lo=lo):
            zero(xe, lo, HALO)
            for row in range(2):
                zero(ry.at[row, pl.ds(PAIRS, PAIRS)], lo, HALO)
    for side in range(2):
        @pl.when(jnp.logical_not(has[1][side]))
        def _(side=side):
            zero(ry.at[side], 0, top + HALO)

    n = 0
    for i in range(3):
        for side in range(2):
            n = n + has[i][side].astype(jnp.int32)
    pl.semaphore_wait(barrier, n)

    def remote(src, dst, k, i, side):
        return pltpu.make_async_remote_copy(
            src_ref=src, dst_ref=dst, send_sem=send_sem.at[k], recv_sem=recv_sem.at[k],
            device_id=peer(i, side), device_id_type=pl.DeviceIdType.MESH,
        )

    def x_copy(side, group):
        span = pl.ds(2 * PAIRS * group, 2 * PAIRS)
        src = xe.at[span, pl.ds(HALO if side == 0 else size_x, HALO)]
        dst = xe.at[span, pl.ds(top if side == 0 else 0, HALO)]
        return remote(src, dst, 2 * group + side, 0, side)

    def y_copy(side, part, group):
        lo, count = ((0, HALO), (HALO, size_x), (top, HALO))[part]
        span = pl.ds(PAIRS * group, PAIRS)
        return remote(
            sy.at[side, span, pl.ds(lo, count)], ry.at[1 - side, span, pl.ds(lo, count)],
            2 * GROUPS + (2 * part + side) * GROUPS + group, 1, side,
        )

    def corner(row, side):
        span = pl.ds(PAIRS, PAIRS)
        return remote(
            ry.at[row, span, pl.ds(HALO if side == 0 else size_x, HALO)],
            ry.at[row, span, pl.ds(top if side == 0 else 0, HALO)],
            8 * GROUPS + 2 + 2 * row + side, 0, side,
        )

    def z_copy(side):
        return remote(az, rz.at[1 - side], 8 * GROUPS + side, 2, side)

    def each(i, action):
        for side in range(2):
            @pl.when(has[i][side])
            def _(side=side):
                action(side)

    for group in range(GROUPS):
        each(0, lambda side: x_copy(side, group).start())
        each(1, lambda side: y_copy(side, 1, group).start())
    each(0, lambda side: x_copy(1 - side, 0).wait_recv())
    loop(0, HALO, functools.partial(pack_y, 0))
    loop(top, top + HALO, functools.partial(pack_y, 0))
    for part in (0, 2):
        each(1, lambda side: y_copy(side, part, 0).start())
    each(1, lambda row: y_copy(1 - row, 1, 1).wait_recv())
    each(1, lambda row: each(0, lambda side: corner(row, side).start()))

    wide = lax.broadcasted_iota(jnp.int32, (2 * HALO + size_y, size_z), 1)

    def fill(xs):
        done = []
        for x in xs:
            for p in range(NARR // 2):
                lo, hi = ry[0, p, x], ry[1, p, x]
                for q in range(2):
                    a = 2 * p + q
                    own = pltpu.roll(xe[a, x], HALO, 0)
                    lo_part = lo if q == 0 else pltpu.roll(lo, HALO, 0)
                    hi_part = hi if q == 1 else pltpu.roll(hi, HALO, 0)
                    done.append((
                        a, x, jnp.where(sub < HALO, lo_part, own),
                        jnp.where(sub < HALO, own, hi_part),
                    ))
        for a, x, low, high in done:
            ext[a, x, 0:size_y] = low
            ext[a, x, size_y : 2 * size_y] = high

    each(1, lambda row: y_copy(1 - row, 1, 0).wait_recv())
    loop(HALO, top, fill)
    each(0, lambda side: x_copy(1 - side, 1).wait_recv())
    for part in (0, 2):
        each(1, lambda row: y_copy(1 - row, part, 0).wait_recv())
    each(1, lambda row: each(0, lambda side: corner(row, 1 - side).wait_recv()))
    loop(0, HALO, fill)
    loop(top, top + HALO, fill)

    planes = top + HALO

    def pack_z(a, _):
        packed = jnp.zeros(wide.shape, jnp.float32)
        for x in range(planes):
            spot = (wide >= x * SLOT) & (wide < (x + 1) * SLOT)
            packed = jnp.where(spot, pltpu.roll(ext[a, x], (x * SLOT + HALO) % size_z, 1), packed)
        az[a] = packed
        return 0

    lax.fori_loop(0, NARR, pack_z, 0)
    each(2, lambda side: z_copy(side).start())
    for side in range(2):
        @pl.when(jnp.logical_not(has[2][side]))
        def _(side=side):
            for a in range(NARR):
                rz[side, a] = jnp.zeros(wide.shape, jnp.float32)
    each(2, lambda side: z_copy(1 - side).wait_recv())

    early = lax.rem(wide, SLOT) < HALO
    for a in range(NARR):
        strip[0, a] = jnp.where(early, rz[0, a], az[a])
        strip[1, a] = jnp.where(early, az[a], rz[1, a])

    rows = 2 * HALO + size_y
    up = lambda v: pltpu.roll(v, rows - 1, 0)
    down = lambda v: pltpu.roll(v, 1, 0)
    zup = lambda v: pltpu.roll(v, size_z - 1, 1)
    zdown = lambda v: pltpu.roll(v, 1, 1)
    xup = lambda v: pltpu.roll(v, size_z - SLOT, 1)
    xdown = lambda v: pltpu.roll(v, SLOT, 1)

    def speed(total):
        return relax / (1.0 + 0.75 * total)

    for s in range(2):
        w = strip[s, 6]
        w = w + xdown(w)
        w = w + down(w)
        if s == 0:
            hz[0] = w
        srate[s] = speed(w + zdown(w))
        for c in range(3):
            sprev[s, c] = strip[s, c]

    first_lane = wide == 0
    last_lane = wide == size_z - 1

    def from_low(v, x):
        return pltpu.roll(v, size_z - HALO + 1 - SLOT * x, 1)

    def from_high(v, x):
        return pltpu.roll(v, size_z - 1 - HALO - SLOT * x, 1)

    def make_terms(x, c, u):
        uz = jnp.where(last_lane, from_high(strip[1, c], x), zup(u))
        return node_terms(u * 0.25, uz * 0.25, up)

    def put_terms(done):
        for x, c, three in done:
            for k in range(3):
                terms[x, 3 * c + k] = three[k]

    def setup(xs):
        us = [(x, c, ext[c, x]) for x in xs for c in range(3)]
        done = [(x, c, make_terms(x, c, u)) for x, c, u in us]
        for x, c, u in us:
            prev[c, x] = u
        put_terms(done)

    def setup_rate(xs):
        done = []
        for x in xs:
            w = ext[6, x - 1] + ext[6, x]
            w = w + down(w)
            done.append(speed(w + jnp.where(first_lane, from_low(hz[0], x), zdown(w))))
        for x, r in zip(xs, done):
            rate[x] = r

    loop(0, planes, setup)
    loop(1, planes - 1, setup_rate)

    omega = None
    for step in range(ITERS):
        if step == 1:
            omega = 2.0 / (2.0 - radius * radius)
        elif step > 1:
            omega = 4.0 / (4.0 - radius * radius * omega)
        last = step == ITERS - 1

        def strips():
            done = []
            for s in range(2):
                low, high = [], []
                for c in range(3):
                    u = strip[s, c] * 0.25
                    t = node_terms(u, zup(u), up)
                    low.append(t)
                    high.append([xup(v) for v in t])
                p = stress(stretch(low, high), strip[s, 6])
                for c in range(3):
                    mine = p[3 * c : 3 * c + 3]
                    minus, plus = node_sums([xdown(v) for v in mine], mine, down)
                    u = strip[s, c]
                    fresh = advance(
                        u, sprev[s, c], strip[s, 3 + c], strip[s, 7], srate[s],
                        minus + zdown(plus), omega,
                    )
                    done.append((s, c, u, plus, fresh))
            for s, c, u, plus, fresh in done:
                if s == 0:
                    hz[c] = plus
                if not last:
                    sprev[s, c] = u
                    strip[s, c] = fresh

        def voxels(x, _):
            low = [[terms[x, 3 * c + k] for k in range(3)] for c in range(3)]
            high = [[terms[x + 1, 3 * c + k] for k in range(3)] for c in range(3)]
            p = stress(stretch(low, high), ext[6, x])
            for k in range(9):
                press[x, k] = p[k]
            return 0

        def nodes(xs):
            done = []
            for x in xs:
                for c in range(3):
                    minus, plus = node_sums(
                        [press[x - 1, 3 * c + k] for k in range(3)],
                        [press[x, 3 * c + k] for k in range(3)],
                        down,
                    )
                    f = minus + jnp.where(first_lane, from_low(hz[c], x), zdown(plus))
                    u = ext[c, x]
                    fresh = advance(u, prev[c, x], ext[3 + c, x], ext[7, x], rate[x], f, omega)
                    done.append((x, c, u, fresh))
            if last:
                for x, c, _, fresh in done:
                    out[c, x - HALO] = fresh[HALO : HALO + size_y]
                return
            later = [(x, c, make_terms(x, c, fresh)) for x, c, _, fresh in done]
            for x, c, u, fresh in done:
                prev[c, x] = u
                ext[c, x] = fresh
            put_terms(later)

        strips()
        lax.fori_loop(step, planes - 1 - step, voxels, 0)
        loop(step + 1, planes - 1 - step, nodes)

    for group in range(GROUPS):
        each(0, lambda side: x_copy(side, group).wait_send())
        each(1, lambda side: y_copy(side, 1, group).wait_send())
    for part in (0, 2):
        each(1, lambda side: y_copy(side, part, 0).wait_send())
    each(1, lambda row: each(0, lambda side: corner(row, side).wait_send()))
    each(2, lambda side: z_copy(side).wait_send())


def per_device(counts, start_disp, inertial, material, pinned, stiffness):
    size_x, size_y, size_z = material.shape
    planes, rows = size_x + 2 * HALO, size_y + 2 * HALO
    assert planes * SLOT == size_z and size_y == 2 * HALO
    vmem = pl.BlockSpec(memory_space=pltpu.VMEM)
    f32 = lambda *shape: pltpu.VMEM(shape, jnp.float32)
    return pl.pallas_call(
        functools.partial(kernel, counts),
        out_shape=jax.ShapeDtypeStruct(start_disp.shape, jnp.float32),
        in_specs=[vmem, vmem, vmem, vmem, pl.BlockSpec(memory_space=pltpu.SMEM)],
        out_specs=vmem,
        scratch_shapes=[
            f32(NARR, planes, size_y, size_z),
            f32(2, NARR // 2, planes, size_y, size_z),
            f32(2, NARR // 2, planes, size_y, size_z),
            f32(NARR, planes, rows, size_z),
            f32(NARR, rows, size_z),
            f32(2, NARR, rows, size_z),
            f32(3, planes, rows, size_z),
            f32(planes, rows, size_z),
            f32(planes, 9, rows, size_z),
            f32(planes, 9, rows, size_z),
            f32(2, NARR, rows, size_z),
            f32(2, 3, rows, size_z),
            f32(2, rows, size_z),
            f32(3, rows, size_z),
            pltpu.SemaphoreType.DMA((8 * GROUPS + 6,)),
            pltpu.SemaphoreType.DMA((8 * GROUPS + 6,)),
        ],
        compiler_params=pltpu.CompilerParams(collective_id=0, has_side_effects=True),
    )(start_disp, inertial, material, pinned, stiffness)


def solution(mesh):
    placed = (
        P(None, "gx", "gy", "gz"),
        P(None, "gx", "gy", "gz"),
        P("gx", "gy", "gz"),
        P("gx", "gy", "gz"),
        P(),
    )
    counts = tuple(mesh.shape[a] for a in AXES)
    return jax.shard_map(
        functools.partial(per_device, counts), mesh=mesh, in_specs=placed,
        out_specs=P(None, "gx", "gy", "gz"), check_vma=False,
    )
```

```python
import functools

import jax
import jax.numpy as jnp
from jax import lax
from jax.experimental import pallas as pl
from jax.experimental.pallas import tpu as pltpu
from jax.sharding import PartitionSpec as P

ITERS = 4
POLAR_STEPS = 6
MATS = 8

relax = 0.6
radius = 0.9
HALO = ITERS
SLOT = 2 * HALO
NARR = 8
GROUPS = 2
PAIRS = NARR // 2 // GROUPS
AXES = ("gx", "gy", "gz")


def loop(lo, hi, body, unroll=2):
    assert (hi - lo) % unroll == 0

    def group(k, _):
        body([lo + k * unroll + i for i in range(unroll)])
        return 0

    lax.fori_loop(0, (hi - lo) // unroll, group, 0)


def node_terms(u, uz, roll_y):
    zs, zd = uz + u, uz - u
    ys, yd = roll_y(zs), roll_y(zd)
    return zs + ys, ys - zs, zd + yd


def stretch(low, high):
    deform = []
    for c in range(3):
        dx = high[c][0] - low[c][0]
        dy = high[c][1] + low[c][1]
        dz = high[c][2] + low[c][2]
        row = [dx, dy, dz]
        row[c] = row[c] + 1.0
        deform.append(row)
    return deform


def stress(deform, w):
    total = None
    for c in range(3):
        for d in range(3):
            sq = deform[c][d] * deform[c][d]
            total = sq if total is None else total + sq
    inv = jnp.minimum(lax.rsqrt(total * (1.0 / 3.0)), 1.0) * (0.5**0.5)
    z = [[deform[c][d] * inv for d in range(3)] for c in range(3)]

    def polar(_, flat):
        z = [flat[3 * c : 3 * c + 3] for c in range(3)]
        s = {}
        for i in range(3):
            for j in range(i, 3):
                s[i, j] = z[0][i] * z[0][j] + z[1][i] * z[1][j] + z[2][i] * z[2][j]
        m = [1.5 - s[i, i] for i in range(3)]
        out = []
        for c in range(3):
            a, b, e = z[c]
            out.append(a * m[0] - b * s[0, 1] - e * s[0, 2])
            out.append(b * m[1] - a * s[0, 1] - e * s[1, 2])
            out.append(e * m[2] - a * s[0, 2] - b * s[1, 2])
        return tuple(out)

    flat = lax.fori_loop(
        0, POLAR_STEPS, polar, tuple(z[c][d] for c in range(3) for d in range(3)), unroll=True
    )
    return [w * (deform[k // 3][k % 3] - flat[k] * (2.0**0.5)) for k in range(9)]


def node_sums(before, here, roll_y):
    a = before[0] - here[0]
    b = before[1] + here[1]
    e = before[2] + here[2]
    g = (a - b) + roll_y(a + b)
    e = e + roll_y(e)
    return g - e, g + e


def advance(u, prev, inert, pin, rate, f, omega):
    target = u - rate * ((u - inert) + f)
    fresh = target if omega is None else omega * (target - prev) + prev
    return jnp.where(pin > 0.0, inert, fresh)


def kernel(
    counts, start, inertial, material, pinned, stiff, out,
    xe, sy, ry, ext, az, rz, prev, rate, terms, press, strip, sprev, srate, hz,
    send_sem, recv_sem,
):
    size_x, size_y, size_z = material.shape
    here = [lax.axis_index(a) for a in AXES]
    has = [[here[i] > 0, here[i] < counts[i] - 1] for i in range(3)]

    sub = lax.broadcasted_iota(jnp.int32, (size_y, size_z), 0)
    lane = lax.broadcasted_iota(jnp.int32, (size_y, size_z), 1)
    inside = ((sub < size_y - 1) | has[1][1]) & ((lane < size_z - 1) | has[2][1])
    quarter = [stiff[i] * 0.25 for i in range(MATS)]

    barrier = pltpu.get_barrier_semaphore()

    def peer(i, side):
        return {AXES[i]: here[i] + (1 if side else -1)}

    for i in range(3):
        for side in range(2):
            @pl.when(has[i][side])
            def _(i=i, side=side):
                pl.semaphore_signal(
                    barrier, inc=1, device_id=peer(i, side), device_id_type=pl.DeviceIdType.MESH
                )

    def faces(first, second):
        low = jnp.where(sub < HALO, first, pltpu.roll(second, HALO, 0))
        high = jnp.where(sub < HALO, pltpu.roll(first, HALO, 0), second)
        return low, high

    def pack_y(group, xs):
        done = [
            (p, x, faces(xe[2 * p, x], xe[2 * p + 1, x]))
            for x in xs for p in range(group * PAIRS, (group + 1) * PAIRS)
        ]
        for p, x, (low, high) in done:
            sy[0, p, x] = low
            sy[1, p, x] = high

    def own_planes(xs):
        done = []
        for x in xs:
            mat = material[x]
            w = jnp.zeros((size_y, size_z), jnp.float32)
            for index in range(MATS):
                w = jnp.where(mat == index, quarter[index], w)
            keep = inside & ((x < size_x - 1) | has[0][1])
            pins = pinned[x] > 0
            inert = [inertial[c, x] for c in range(3)]
            arrays = [jnp.where(pins, inert[c], start[c, x]) for c in range(3)] + inert
            arrays += [jnp.where(keep, w, 0.0), jnp.where(pins, 1.0, 0.0)]
            done.append((x + HALO, arrays))
        for x, arrays in done:
            for a in range(NARR):
                xe[a, x] = arrays[a]
            for p in range(NARR // 2):
                low, high = faces(arrays[2 * p], arrays[2 * p + 1])
                sy[0, p, x] = low
                sy[1, p, x] = high

    loop(0, size_x, own_planes, 4)

    def zero(ref, lo, n):
        def body(x, _):
            for a in range(ref.shape[0]):
                ref[a, x] = jnp.zeros(ref.shape[2:], jnp.float32)
            return 0
        lax.fori_loop(lo, lo + n, body, 0)

    top = HALO + size_x
    for side, lo in ((0, 0), (1, top)):
        @pl.when(jnp.logical_not(has[0][side]))
        def _(lo=lo):
            zero(xe, lo, HALO)
            for row in range(2):
                zero(ry.at[row, pl.ds(PAIRS, PAIRS)], lo, HALO)
    for side in range(2):
        @pl.when(jnp.logical_not(has[1][side]))
        def _(side=side):
            zero(ry.at[side], 0, top + HALO)

    n = 0
    for i in range(3):
        for side in range(2):
            n = n + has[i][side].astype(jnp.int32)
    pl.semaphore_wait(barrier, n)

    def remote(src, dst, k, i, side):
        return pltpu.make_async_remote_copy(
            src_ref=src, dst_ref=dst, send_sem=send_sem.at[k], recv_sem=recv_sem.at[k],
            device_id=peer(i, side), device_id_type=pl.DeviceIdType.MESH,
        )

    def x_copy(side, group):
        span = pl.ds(2 * PAIRS * group, 2 * PAIRS)
        src = xe.at[span, pl.ds(HALO if side == 0 else size_x, HALO)]
        dst = xe.at[span, pl.ds(top if side == 0 else 0, HALO)]
        return remote(src, dst, 2 * group + side, 0, side)

    def y_copy(side, part, group):
        lo, count = ((0, HALO), (HALO, size_x), (top, HALO))[part]
        span = pl.ds(PAIRS * group, PAIRS)
        return remote(
            sy.at[side, span, pl.ds(lo, count)], ry.at[1 - side, span, pl.ds(lo, count)],
            2 * GROUPS + (2 * part + side) * GROUPS + group, 1, side,
        )

    def corner(row, side):
        span = pl.ds(PAIRS, PAIRS)
        return remote(
            ry.at[row, span, pl.ds(HALO if side == 0 else size_x, HALO)],
            ry.at[row, span, pl.ds(top if side == 0 else 0, HALO)],
            8 * GROUPS + 2 + 2 * row + side, 0, side,
        )

    def z_copy(side):
        return remote(az, rz.at[1 - side], 8 * GROUPS + side, 2, side)

    def each(i, action):
        for side in range(2):
            @pl.when(has[i][side])
            def _(side=side):
                action(side)

    for group in range(GROUPS):
        each(0, lambda side: x_copy(side, group).start())
        each(1, lambda side: y_copy(side, 1, group).start())
    each(0, lambda side: x_copy(1 - side, 0).wait_recv())
    loop(0, HALO, functools.partial(pack_y, 0), HALO)
    loop(top, top + HALO, functools.partial(pack_y, 0), HALO)
    for part in (0, 2):
        each(1, lambda side: y_copy(side, part, 0).start())
    each(1, lambda row: y_copy(1 - row, 1, 1).wait_recv())
    each(1, lambda row: each(0, lambda side: corner(row, side).start()))

    wide = lax.broadcasted_iota(jnp.int32, (2 * HALO + size_y, size_z), 1)

    def fill(xs):
        done = []
        for x in xs:
            for p in range(NARR // 2):
                lo, hi = ry[0, p, x], ry[1, p, x]
                for q in range(2):
                    a = 2 * p + q
                    own = pltpu.roll(xe[a, x], HALO, 0)
                    lo_part = lo if q == 0 else pltpu.roll(lo, HALO, 0)
                    hi_part = hi if q == 1 else pltpu.roll(hi, HALO, 0)
                    done.append((
                        a, x, jnp.where(sub < HALO, lo_part, own),
                        jnp.where(sub < HALO, own, hi_part),
                    ))
        for a, x, low, high in done:
            ext[a, x, 0:size_y] = low
            ext[a, x, size_y : 2 * size_y] = high

    each(1, lambda row: y_copy(1 - row, 1, 0).wait_recv())
    loop(HALO, top, fill, 4)
    each(0, lambda side: x_copy(1 - side, 1).wait_recv())
    for part in (0, 2):
        each(1, lambda row: y_copy(1 - row, part, 0).wait_recv())
    each(1, lambda row: each(0, lambda side: corner(row, 1 - side).wait_recv()))
    loop(0, HALO, fill, HALO)
    loop(top, top + HALO, fill, HALO)

    planes = top + HALO

    def pack_z(arrays):
        packed = [jnp.zeros(wide.shape, jnp.float32) for _ in arrays]
        for x in range(planes):
            spot = (wide >= x * SLOT) & (wide < (x + 1) * SLOT)
            for k, a in enumerate(arrays):
                moved = pltpu.roll(ext[a, x], (x * SLOT + HALO) % size_z, 1)
                packed[k] = jnp.where(spot, moved, packed[k])
        for a, value in zip(arrays, packed):
            az[a] = value

    loop(0, NARR, pack_z, 4)
    each(2, lambda side: z_copy(side).start())

    rows = 2 * HALO + size_y
    up = lambda v: pltpu.roll(v, rows - 1, 0)
    down = lambda v: pltpu.roll(v, 1, 0)
    zup = lambda v: pltpu.roll(v, size_z - 1, 1)
    zdown = lambda v: pltpu.roll(v, 1, 1)

    def begin(xs):
        us = [(x, c, ext[c, x]) for x in xs for c in range(3)]
        for x, c, u in us:
            prev[c, x] = u

    def weigh(xs):
        sums = [ext[6, x - 1] + ext[6, x] for x in xs]
        sums = [w + down(w) for w in sums]
        for x, w in zip(xs, sums):
            rate[x] = w

    loop(0, planes, begin, 4)
    loop(1, planes - 1, weigh, (planes - 2) // 2)
    for side in range(2):
        @pl.when(jnp.logical_not(has[2][side]))
        def _(side=side):
            for a in range(NARR):
                rz[side, a] = jnp.zeros(wide.shape, jnp.float32)
    each(2, lambda side: z_copy(1 - side).wait_recv())

    early = lax.rem(wide, SLOT) < HALO
    for a in range(NARR):
        strip[0, a] = jnp.where(early, rz[0, a], az[a])
        strip[1, a] = jnp.where(early, az[a], rz[1, a])

    xup = lambda v: pltpu.roll(v, size_z - SLOT, 1)
    xdown = lambda v: pltpu.roll(v, SLOT, 1)

    def speed(total):
        return relax / (1.0 + 0.75 * total)

    for s in range(2):
        w = strip[s, 6]
        w = w + xdown(w)
        w = w + down(w)
        if s == 0:
            hz[0] = w
        srate[s] = speed(w + zdown(w))
        for c in range(3):
            sprev[s, c] = strip[s, c]

    first_lane = wide == 0
    last_lane = wide == size_z - 1

    def from_low(v, x):
        return pltpu.roll(v, size_z - HALO + 1 - SLOT * x, 1)

    def from_high(v, x):
        return pltpu.roll(v, size_z - 1 - HALO - SLOT * x, 1)

    def make_terms(x, c, u):
        uz = jnp.where(last_lane, from_high(strip[1, c], x), zup(u))
        return node_terms(u * 0.25, uz * 0.25, up)

    def put_terms(done):
        for x, c, three in done:
            for k in range(3):
                terms[x, 3 * c + k] = three[k]

    def setup(xs):
        us = [(x, c, ext[c, x]) for x in xs for c in range(3)]
        done = [(x, c, make_terms(x, c, u)) for x, c, u in us]
        put_terms(done)

    def setup_rate(xs):
        done = []
        for x in xs:
            w = rate[x]
            done.append(speed(w + jnp.where(first_lane, from_low(hz[0], x), zdown(w))))
        for x, r in zip(xs, done):
            rate[x] = r

    loop(0, planes, setup, 4)
    loop(1, planes - 1, setup_rate, (planes - 2) // 2)

    omega = None
    for step in range(ITERS):
        if step == 1:
            omega = 2.0 / (2.0 - radius * radius)
        elif step > 1:
            omega = 4.0 / (4.0 - radius * radius * omega)
        last = step == ITERS - 1

        def strips():
            done = []
            for s in range(2):
                low, high = [], []
                for c in range(3):
                    u = strip[s, c] * 0.25
                    t = node_terms(u, zup(u), up)
                    low.append(t)
                    high.append([xup(v) for v in t])
                p = stress(stretch(low, high), strip[s, 6])
                for c in range(3):
                    mine = p[3 * c : 3 * c + 3]
                    minus, plus = node_sums([xdown(v) for v in mine], mine, down)
                    u = strip[s, c]
                    fresh = advance(
                        u, sprev[s, c], strip[s, 3 + c], strip[s, 7], srate[s],
                        minus + zdown(plus), omega,
                    )
                    done.append((s, c, u, plus, fresh))
            for s, c, u, plus, fresh in done:
                if s == 0:
                    hz[c] = plus
                if not last:
                    sprev[s, c] = u
                    strip[s, c] = fresh

        def voxels(x, _):
            low = [[terms[x, 3 * c + k] for k in range(3)] for c in range(3)]
            high = [[terms[x + 1, 3 * c + k] for k in range(3)] for c in range(3)]
            p = stress(stretch(low, high), ext[6, x])
            for k in range(9):
                press[x, k] = p[k]
            return 0

        def nodes(xs):
            done = []
            for x in xs:
                for c in range(3):
                    minus, plus = node_sums(
                        [press[x - 1, 3 * c + k] for k in range(3)],
                        [press[x, 3 * c + k] for k in range(3)],
                        down,
                    )
                    f = minus + jnp.where(first_lane, from_low(hz[c], x), zdown(plus))
                    u = ext[c, x]
                    fresh = advance(u, prev[c, x], ext[3 + c, x], ext[7, x], rate[x], f, omega)
                    done.append((x, c, u, fresh))
            if last:
                for x, c, _, fresh in done:
                    out[c, x - HALO] = fresh[HALO : HALO + size_y]
                return
            later = [(x, c, make_terms(x, c, fresh)) for x, c, _, fresh in done]
            for x, c, u, fresh in done:
                prev[c, x] = u
                ext[c, x] = fresh
            put_terms(later)

        strips()
        lax.fori_loop(step, planes - 1 - step, voxels, 0)
        loop(step + 1, planes - 1 - step, nodes)

    for group in range(GROUPS):
        each(0, lambda side: x_copy(side, group).wait_send())
        each(1, lambda side: y_copy(side, 1, group).wait_send())
    for part in (0, 2):
        each(1, lambda side: y_copy(side, part, 0).wait_send())
    each(1, lambda row: each(0, lambda side: corner(row, side).wait_send()))
    each(2, lambda side: z_copy(side).wait_send())


def per_device(counts, start_disp, inertial, material, pinned, stiffness):
    size_x, size_y, size_z = material.shape
    planes, rows = size_x + 2 * HALO, size_y + 2 * HALO
    assert planes * SLOT == size_z and size_y == 2 * HALO
    vmem = pl.BlockSpec(memory_space=pltpu.VMEM)
    f32 = lambda *shape: pltpu.VMEM(shape, jnp.float32)
    return pl.pallas_call(
        functools.partial(kernel, counts),
        out_shape=jax.ShapeDtypeStruct(start_disp.shape, jnp.float32),
        in_specs=[vmem, vmem, vmem, vmem, pl.BlockSpec(memory_space=pltpu.SMEM)],
        out_specs=vmem,
        scratch_shapes=[
            f32(NARR, planes, size_y, size_z),
            f32(2, NARR // 2, planes, size_y, size_z),
            f32(2, NARR // 2, planes, size_y, size_z),
            f32(NARR, planes, rows, size_z),
            f32(NARR, rows, size_z),
            f32(2, NARR, rows, size_z),
            f32(3, planes, rows, size_z),
            f32(planes, rows, size_z),
            f32(planes, 9, rows, size_z),
            f32(planes, 9, rows, size_z),
            f32(2, NARR, rows, size_z),
            f32(2, 3, rows, size_z),
            f32(2, rows, size_z),
            f32(3, rows, size_z),
            pltpu.SemaphoreType.DMA((8 * GROUPS + 6,)),
            pltpu.SemaphoreType.DMA((8 * GROUPS + 6,)),
        ],
        compiler_params=pltpu.CompilerParams(collective_id=0, has_side_effects=True),
    )(start_disp, inertial, material, pinned, stiffness)


def solution(mesh):
    placed = (
        P(None, "gx", "gy", "gz"),
        P(None, "gx", "gy", "gz"),
        P("gx", "gy", "gz"),
        P("gx", "gy", "gz"),
        P(),
    )
    counts = tuple(mesh.shape[a] for a in AXES)
    return jax.shard_map(
        functools.partial(per_device, counts), mesh=mesh, in_specs=placed,
        out_specs=P(None, "gx", "gy", "gz"), check_vma=False,
    )
```
